32 devices in a mesh: freq: 4 (over x, core), rec: 8 (over z, y).
Axes of the slice: x: 2, y: 2, z: 4, core: 2. Of those that a mesh axis runs over, the one named last changes fastest.
Arguments:
- response_real: float32 [96, 1536, 1536], P('freq', 'rec'), may hold values from -0.109375 to 0.109375
- response_imaginary: float32 [96, 1536, 1536], P('freq', 'rec'), may hold values from -0.109375 to 0.109375
- focus: float32 [1536, 96, 128], P('rec', 'freq'), may hold values from -6 to 6
- initial: float32 [1536, 96, 128], P('rec', 'freq'), may hold values from -6 to 6
- onset: int32 [1536, 64], P('rec'), may hold values from 24 to 167
Outputs:
- focus_next: float32 [1536, 96, 128], P('rec', 'freq')
The draws below stay inside these ranges and needn't reach their ends.
All inputs are finite; a program needn't handle non-finite values.
Results may differ from the reference program's by a relative error of at most 0.0003.
Values sent between devices are 32-bit elements; how exact they have to be, the bound alone decides.
No kernel may reach another device: no remote copies, remote signals or barrier semaphores. Data moves between devices by JAX's collectives and lax.ppermute only.
A program may use at most 192 MiB of HBM per device.

```python
import math
import jax
import jax.numpy as jnp
from jax import lax

F = 96
NPOS = 1536
P_SIZE = 64
NT = 192


def set_ends(drawn, own_key, least, top_value):
    dims = drawn.shape
    place = [jax.random.randint(jax.random.fold_in(own_key, axis), (), 0, dims[axis]) for axis in range(len(dims))]
    drawn = drawn.at[tuple(place)].set(least)
    longest = dims.index(max(dims))
    place[longest] = (place[longest] + 1) % dims[longest]
    return drawn.at[tuple(place)].set(top_value)


def shard_levels(stream_key, shape, pieces, smallest, top_value):
    factor_of = 1.0
    for axis_at, blocks in pieces:
        steps = jax.random.uniform(jax.random.fold_in(jax.random.fold_in(stream_key, 6), axis_at), (blocks,), jnp.float32, smallest / len(pieces), top_value / len(pieces))
        factor_of = factor_of * jnp.repeat(jnp.exp(steps), shape[axis_at] // blocks).reshape((-1,) + (1,) * (len(shape) - 1 - axis_at))
    return factor_of


def scatter_about(stream_key, dims, spread, most, cuts=(), held_as=jnp.bfloat16):
    level = shard_levels(stream_key, dims, cuts, -0.22, 0.18) if cuts else 1.0
    values = jax.random.normal(stream_key, dims, jnp.float32) * spread * level
    return jnp.minimum(jnp.maximum(values, -most), most).astype(held_as)


def setup_inputs(seed: int = 0) -> dict:
    key_of = jax.random.split(jax.random.key(seed), 6)
    return {
        "response_real": scatter_about(key_of[0], (F, NPOS, NPOS), (2 * NPOS) ** -0.5, 0.109375, ((0, 4), (1, 8)), jnp.float32),
        "response_imaginary": scatter_about(key_of[1], (F, NPOS, NPOS), (2 * NPOS) ** -0.5, 0.109375, ((0, 4), (1, 8)), jnp.float32),
        "focus": scatter_about(key_of[2], (NPOS, F, 2 * P_SIZE), 1.0, 6.0, ((0, 8), (1, 4)), jnp.float32),
        "initial": scatter_about(key_of[3], (NPOS, F, 2 * P_SIZE), 1.0, 6.0, ((0, 8), (1, 4)), jnp.float32),
        "onset": set_ends(jax.random.randint(key_of[4], (NPOS, P_SIZE), NT // 8, NT - NT // 8), jax.random.fold_in(key_of[4], 1), NT // 8, (NT - NT // 8) - 1).astype(jnp.int32),
    }


def tables(freqs):
    samples = 2 * freqs
    order = lax.iota(jnp.int32, freqs)
    sample = lax.iota(jnp.int32, samples)
    phase = (order[:, None] * sample[None, :]) % samples
    phases = (2.0 * math.pi / samples) * phase.astype(jnp.float32)
    cosine = jnp.cos(phases)
    sine = jnp.sin(phases)
    factor = jnp.where(order == 0, 1.0, 2.0).astype(jnp.float32)[:, None] / samples
    inverse = jnp.stack([factor * cosine, -factor * sine])
    forward = jnp.stack([cosine, -sine])
    return inverse, forward, sample


def window(spectrum, onset):
    count, freqs, width = spectrum.shape
    half = width // 2
    inverse, forward, sample = tables(freqs)
    split = spectrum.reshape(count, freqs, 2, half)
    traces = jnp.einsum("nkcp,ckt->ntp", split, inverse, precision=lax.Precision.HIGHEST)
    keep = sample[None, :, None] < onset[:, None, :]
    clipped = jnp.where(keep, traces, 0.0)
    back = jnp.einsum("ntp,ckt->nkcp", clipped, forward, precision=lax.Precision.HIGHEST)
    return back.reshape(count, freqs, width)


def adjoint_terms(real_part, imag_part, values):
    half = values.shape[2] // 2
    first = jnp.einsum("frs,rfq->sfq", real_part, values, precision=lax.Precision.HIGHEST)
    second = jnp.einsum("frs,rfq->sfq", imag_part, values, precision=lax.Precision.HIGHEST)
    return jnp.concatenate([first[..., :half] + second[..., half:], first[..., half:] - second[..., :half]], axis=2)


def forward_terms(real_part, imag_part, values):
    half = values.shape[2] // 2
    first = jnp.einsum("frs,sfq->rfq", real_part, values, precision=lax.Precision.HIGHEST)
    second = jnp.einsum("frs,sfq->rfq", imag_part, values, precision=lax.Precision.HIGHEST)
    return jnp.concatenate([first[..., :half] - second[..., half:], first[..., half:] + second[..., :half]], axis=2)


def reference(response_real, response_imaginary, focus, initial, onset):
    adjoint = adjoint_terms(response_real, response_imaginary, focus)
    windowed = window(adjoint, onset)
    forward = forward_terms(response_real, response_imaginary, windowed)
    return initial - window(forward, onset)
```

```python
import functools
import math

import jax
import jax.numpy as jnp
import numpy as np
from jax import lax
from jax.experimental import pallas as pl
from jax.experimental.pallas import tpu as pltpu
from jax.sharding import PartitionSpec as P

CHUNKS = 2
DEPTH = 4
UNIT = 2
F32, BF16 = jnp.float32, jnp.bfloat16


def ring_order(mesh):
    axis = mesh.axis_names.index("rec")
    devices = np.moveaxis(mesh.devices, axis, 0).reshape(mesh.devices.shape[axis], -1)[:, 0]
    count = len(devices)
    try:
        spots = {tuple(d.coords[1:]): i for i, d in enumerate(devices)}
    except AttributeError:
        return list(range(count))
    ys = sorted({y for y, _ in spots})
    zs = sorted({z for _, z in spots})
    if len(spots) != count or len(ys) * len(zs) != count or len(ys) % 2 or len(zs) < 2:
        return list(range(count))
    path = [(y, zs[0]) for y in ys]
    for turn, y in enumerate(reversed(ys)):
        path += [(y, z) for z in (zs[1:] if turn % 2 == 0 else zs[:0:-1])]
    return [spots[p] for p in path]


def tiling(width):
    return (width // 128, 128) if width % 128 == 0 else (1, width)


def split(x):
    high = x.astype(BF16)
    return high, (x - high.astype(F32)).astype(BF16)


def dot(a, b, dims=((1,), (0,))):
    return lax.dot_general(a, b, (dims, ((), ())), preferred_element_type=F32)


def adjoint_kernel(start, width, groups, real_hbm, imag_hbm, x_ref, out_ref, real_ref, imag_ref, sems):
    f = pl.program_id(0)
    blocks, _, tiles, _, pair, lanes = out_ref.shape
    cols = tiles * lanes
    each = pair // 2
    half = x_ref.shape[2] // 2
    x = x_ref[:, pl.ds(f, 1), :].reshape(x_ref.shape[0], 2 * half).T
    re, im = x[start:start + width], x[half + start:half + start + width]
    left = jnp.concatenate([jnp.concatenate([re, im], 1), jnp.concatenate([im, -re], 1)], 0)
    high, low = split(left)
    left = jnp.concatenate(
        [jnp.concatenate([high, high], 1), jnp.concatenate([low, jnp.zeros_like(low)], 1)], 0
    )
    sources = [lambda n, ref=ref: ref.at[n] for ref in (real_hbm, imag_hbm)]
    slot, = stream(0, real_hbm.shape[0], 1, sources, (real_ref, imag_ref), sems)
    for g in range(groups):
        at = pl.ds(g * cols, cols)
        right = jnp.concatenate([real_ref[slot, :, at], imag_ref[slot, :, at]], 0)
        right = jnp.concatenate(split(right), 0)
        both = dot(left, right)
        total = both[: 2 * width] + both[2 * width:]
        for i in range(blocks):
            for c in range(2):
                row = c * width + i * each
                for t in range(tiles):
                    out_ref[i, g, t, 0, c * each:(c + 1) * each, :] = total[
                        row:row + each, t * lanes:(t + 1) * lanes
                    ]


def stream(first, count, unit, sources, buffers, sems):
    depth = buffers[0].shape[0]
    step = pl.program_id(0)
    ahead = min(depth - unit, count)

    def copies(f):
        slot = lax.rem(f, depth)
        return [
            pltpu.make_async_copy(source(f + first), buffer.at[slot], sems.at[n, slot])
            for n, (source, buffer) in enumerate(zip(sources, buffers))
        ]

    @pl.when(step == 0)
    def _():
        for f in range(ahead):
            for copy in copies(jnp.int32(f)):
                copy.start()

    for u in range(unit):
        later = step * unit + ahead + u

        @pl.when(later < count)
        def _():
            for copy in copies(later):
                copy.start()

    for u in range(unit):
        for copy in copies(step * unit + u):
            copy.wait()
    return [lax.rem(step * unit + u, depth) for u in range(unit)]


def unit_of(count):
    return UNIT if count % UNIT == 0 else 1


def adjoint_terms(real_part, imag_part, x, start, width, blocks, groups):
    freqs, rows, cols = real_part.shape
    each = width // blocks
    tiles, lanes = tiling(cols // groups)
    whole = pl.BlockSpec(memory_space=pl.ANY)
    return pl.pallas_call(
        functools.partial(adjoint_kernel, start, width, groups),
        grid=(freqs,),
        in_specs=[whole, whole, pl.BlockSpec(x.shape, lambda f: (0, 0, 0))],
        out_specs=pl.BlockSpec((blocks, groups, tiles, 1, 2 * each, lanes), lambda f: (0, 0, 0, f, 0, 0)),
        out_shape=jax.ShapeDtypeStruct((blocks, groups, tiles, freqs, 2 * each, lanes), F32),
        scratch_shapes=[pltpu.VMEM((DEPTH, rows, cols), F32)] * 2 + [pltpu.SemaphoreType.DMA((2, DEPTH))],
        compiler_params=pltpu.CompilerParams(dimension_semantics=("arbitrary",)),
        cost_estimate=pl.CostEstimate(
            flops=24 * width * freqs * rows * cols, bytes_accessed=8 * freqs * rows * cols, transcendentals=0
        ),
        name="adjoint",
    )(real_part, imag_part, x)


def window_kernel(x_ref, onset_ref, inv_ref, fwd_ref, out_ref):
    groups, tiles, _, lanes = x_ref.shape
    each = onset_ref.shape[0]
    order = x_ref.shape[2] // each
    inverse = inv_ref[...]
    forward = fwd_ref[...]
    samples = inv_ref.shape[0] // 2
    when = lax.broadcasted_iota(jnp.int32, (samples, tiles * lanes), 0)

    def rows(p):
        return pl.ds(p, order, stride=each) if each > 1 else pl.ds(0, order)

    def apply(matrix, value):
        count = matrix.shape[0] // 2
        high, low = split(value)
        both = dot(matrix, high)
        return both[:count] + both[count:] + dot(matrix[:count], low)

    for p in range(each):
        spectra = jnp.concatenate(
            [jnp.concatenate([x_ref[g, t, rows(p), :] for t in range(tiles)], 1) for g in range(groups)], 0
        )
        traces = apply(inverse, spectra)
        clipped = jnp.where(when < onset_ref[p:p + 1, :], traces, 0.0)
        back = apply(forward, clipped)
        for g in range(groups):
            for t in range(tiles):
                out_ref[g, t, rows(p), :] = back[g * order:(g + 1) * order, t * lanes:(t + 1) * lanes]


def window_tables(freqs):
    samples = 2 * freqs
    k, t = np.arange(freqs), np.arange(samples)
    phase = 2.0 * np.pi / samples * (k[:, None] * t[None, :] % samples)
    factor = np.where(k == 0, 1.0, 2.0)[:, None] / samples
    inverse = np.stack([factor * np.cos(phase), -factor * np.sin(phase)], 1)
    forward = np.stack([np.cos(phase), -np.sin(phase)], 1)
    inverse = inverse.reshape(2 * freqs, samples).T
    forward = forward.reshape(2 * freqs, samples)

    def stacked(m):
        m = m.astype(np.float32)
        high = m.astype(BF16)
        low = (m - high.astype(np.float32)).astype(BF16)
        return np.concatenate([high, low], 0)

    return stacked(inverse), stacked(forward)


def window(x, onset, inverse, forward):
    groups, tiles, freqs, pair, lanes = x.shape
    flat = x.reshape(groups, tiles, freqs * pair, lanes)
    vmem = pl.BlockSpec(memory_space=pltpu.VMEM)
    out = pl.pallas_call(
        window_kernel,
        out_shape=jax.ShapeDtypeStruct(flat.shape, F32),
        in_specs=[vmem] * 4,
        out_specs=vmem,
        cost_estimate=pl.CostEstimate(
            flops=24 * groups * freqs * flat.size, bytes_accessed=8 * flat.size, transcendentals=0
        ),
        name="window",
    )(flat, onset, inverse, forward)
    return out.reshape(x.shape)


def pieces_of(freqs):
    return [(0, freqs - 8), (freqs - 8, 8)] if freqs % 8 == 0 and freqs > 8 else [(0, freqs)]


def combine(total, rows, blocks, each):
    count = blocks * 2 * each
    high, low = total[:, :count], total[:, count:]
    parts = [high[n:n + rows] + low[n:n + rows] + high[n + rows:n + 2 * rows] for n in (0, 2 * rows)]
    both = jnp.concatenate(parts, 1).T
    first, second = both[:count], both[count:].reshape(blocks, 2 * each, rows)
    turned = jnp.concatenate([-second[:, each:], second[:, :each]], 1)
    return first + turned.reshape(count, rows)


def strips_of(freqs):
    return [(n, 8) for n in range(0, freqs, 8)] if freqs % 8 == 0 else [(0, freqs)]


def forward_kernel(relative, groups, first, number, d_ref, real_hbm, imag_hbm, w_hbm, *refs):
    outs, (result_ref, real_ref, imag_ref, w_ref, sems) = refs[-5 - groups:-5], refs[-5:]
    unit = unit_of(number)
    sources = [lambda n, ref=ref: ref.at[n] for ref in (real_hbm, imag_hbm)]
    sources.append(lambda n: w_hbm.at[:, :, :, n])
    slots = stream(first, number, unit, sources, (real_ref, imag_ref, w_ref), sems)
    _, blocks, _, tiles, pair, lanes = w_ref.shape
    part = tiles * lanes
    rows = real_hbm.shape[1]
    count = blocks * pair
    for u, slot in enumerate(slots):
        w = jnp.concatenate([w_ref[slot, :, g, t] for g in range(groups) for t in range(tiles)], 2)
        right = jnp.concatenate(split(w.reshape(count, groups * part)), 0)
        left = jnp.concatenate([*split(real_ref[slot]), *split(imag_ref[slot])], 0)
        result_ref[u] = combine(dot(left, right, ((1,), (1,))), rows, blocks, pair // 2)
    per = blocks // groups
    d = d_ref[0] if relative else 0
    for u in range(unit):
        for k, out_ref in enumerate(outs):
            out_tiles, _, _, out_lanes = out_ref.shape
            start = member(d, k, per * pair)
            value = result_ref[u, pl.ds(start, per * pair), :]
            wide = jnp.concatenate([value[i * pair:(i + 1) * pair] for i in range(per)], 1)
            for t in range(out_tiles):
                out_ref[t, pl.program_id(0) * unit + u] = wide[:, t * out_lanes:(t + 1) * out_lanes]


def member(d, k, size, offset=0):
    start = (d ^ k) * size + offset
    return start if isinstance(d, int) else pl.multiple_of(start, 8)


def forward_terms(relative, d, real_part, imag_part, w, after, first, count):
    _, rows, cols = real_part.shape
    blocks, groups, tiles, _, pair, lanes = w.shape
    out_tiles, out_lanes = tiling(blocks // groups * rows)
    unit = unit_of(count)
    depth = DEPTH + unit - 1
    whole = pl.BlockSpec(memory_space=pl.ANY)
    return pl.pallas_call(
        functools.partial(forward_kernel, relative, groups, first, count),
        grid=(count // unit,),
        in_specs=[pl.BlockSpec(memory_space=pltpu.SMEM)] + [whole] * (3 + len(after)),
        out_specs=[pl.BlockSpec((out_tiles, count, pair, out_lanes), lambda f: (0, 0, 0, 0))] * groups,
        out_shape=[jax.ShapeDtypeStruct((out_tiles, count, pair, out_lanes), F32)] * groups,
        scratch_shapes=[
            pltpu.VMEM((unit, blocks * pair, rows), F32),
            pltpu.VMEM((depth, rows, cols), F32),
            pltpu.VMEM((depth, rows, cols), F32),
            pltpu.VMEM((depth, blocks, groups, tiles, pair, lanes), F32),
            pltpu.SemaphoreType.DMA((3, depth)),
        ],
        compiler_params=pltpu.CompilerParams(dimension_semantics=("arbitrary",)),
        cost_estimate=pl.CostEstimate(
            flops=12 * blocks * pair * count * rows * cols, bytes_accessed=8 * count * rows * cols, transcendentals=0
        ),
        name="forward",
    )(d, real_part, imag_part, w, *after)


def window_pieces_kernel(relative, groups, chunk, pieces, strips, d_ref, onset_ref, inv_ref, fwd_ref, *refs):
    number = groups * len(pieces)
    ins, outs, spectra_ref = refs[:number], refs[number:-1], refs[-1]
    tiles, _, lanes = ins[0].shape
    each = onset_ref.shape[1]
    freqs = sum(count for _, count in pieces)
    inverse = inv_ref[...]
    forward = fwd_ref[...]
    samples = inv_ref.shape[0] // 2
    when = lax.broadcasted_iota(jnp.int32, (samples, tiles * lanes), 0)
    d = d_ref[0] if relative else 0

    def apply(matrix, value):
        count = matrix.shape[0] // 2
        high, low = split(value)
        both = dot(matrix, high)
        return both[:count] + both[count:] + dot(matrix[:count], low)

    def places(cuts):
        return [
            (h * groups + k, pl.ds(member(d, k, 2 * freqs, 2 * first), 2 * count), 2 * count)
            for h, (first, count) in enumerate(cuts)
            for k in range(groups)
        ]

    for p in range(each):
        for n, place, order in places(pieces):
            rows = pl.ds(p, order, stride=each) if each > 1 else pl.ds(0, order)
            for t in range(tiles):
                spectra_ref[p, place, t * lanes:(t + 1) * lanes] = ins[n][t, rows, :]
        traces = apply(inverse, spectra_ref[p])
        clipped = jnp.where(when < onset_ref[chunk, p:p + 1, :], traces, 0.0)
        spectra_ref[p] = apply(forward, clipped)
        for n, place, order in places(strips):
            rows = pl.ds(p, order, stride=each) if each > 1 else pl.ds(0, order)
            for t in range(tiles):
                outs[n][t, rows, :] = spectra_ref[p, place, t * lanes:(t + 1) * lanes]


def window_pieces(relative, d, parts, chunk, onset, inverse, forward, pieces, strips):
    groups = len(parts[0])
    flat = [x.reshape(x.shape[0], -1, x.shape[3]) for piece in parts for x in piece]
    tiles, _, lanes = flat[0].shape
    each = onset.shape[1]
    vmem = pl.BlockSpec(memory_space=pltpu.VMEM)
    size = sum(x.size for x in flat)
    shapes = [(tiles, count, 2 * each, lanes) for _, count in strips for _ in range(groups)]
    flat_shapes = [jax.ShapeDtypeStruct((tiles, count * 2 * each, lanes), F32) for _, count, _, _ in shapes]
    out = pl.pallas_call(
        functools.partial(window_pieces_kernel, relative, groups, chunk, pieces, strips),
        out_shape=flat_shapes,
        in_specs=[pl.BlockSpec(memory_space=pltpu.SMEM)] + [vmem] * (3 + len(flat)),
        out_specs=[vmem] * len(shapes),
        scratch_shapes=[pltpu.VMEM((each, inverse.shape[1], tiles * lanes), F32)],
        cost_estimate=pl.CostEstimate(
            flops=12 * inverse.shape[1] * size, bytes_accessed=8 * size, transcendentals=0
        ),
        name="window",
    )(d, onset, inverse, forward, *flat)
    out = [x.reshape(shape) for x, shape in zip(out, shapes)]
    return [out[h * groups:(h + 1) * groups] for h in range(len(strips))]


def finish_kernel(relative, chunks, groups, d_ref, initial_ref, before_ref, *refs):
    del before_ref
    parts, out_ref, turned_ref = refs[:chunks * groups], refs[-2], refs[-1]
    tiles, freqs, pair, lanes = parts[0].shape
    rows, _, full = out_ref.shape
    each, per, half = pair // 2, tiles * lanes // rows, full // 2
    d = d_ref[0] if relative else 0
    for f in range(freqs):
        for j in range(chunks):
            for k in range(groups):
                part = parts[j * groups + k]
                value = jnp.concatenate([part[t, f] for t in range(tiles)], 1)
                for c in range(2):
                    block = jnp.concatenate(
                        [value[c * each:(c + 1) * each, i * rows:(i + 1) * rows] for i in range(per)], 0
                    )
                    start = member(d, k, per * each, c * half + j * half // chunks)
                    turned_ref[f, pl.ds(start, per * each), :] = block
        out_ref[:, f, :] = initial_ref[:, f, :] - turned_ref[f].T


def finish(relative, d, initial, before, parts, first, count):
    rows, freqs, full = initial.shape
    chunks, groups = len(parts), len(parts[0])
    vmem = pl.BlockSpec(memory_space=pltpu.VMEM)
    strip = pl.BlockSpec((rows, count, full), lambda i: (0, first // count, 0))
    return pl.pallas_call(
        functools.partial(finish_kernel, relative, chunks, groups),
        grid=(1,),
        out_shape=jax.ShapeDtypeStruct(initial.shape, F32),
        in_specs=[pl.BlockSpec(memory_space=pltpu.SMEM), strip, pl.BlockSpec(memory_space=pl.ANY)]
        + [vmem] * (chunks * groups),
        out_specs=strip,
        scratch_shapes=[pltpu.VMEM((count, full, rows), F32)],
        input_output_aliases={} if before is initial else {2: 0},
        name="finish",
    )(d, initial, before, *[x for part in parts for x in part])


def swap(relative, parts):
    groups = len(parts)
    if not relative:
        return list(exchange(jnp.stack(parts)))
    return [
        lax.ppermute(x, "freq", [(i, i ^ k) for i in range(groups)]) if k else x for k, x in enumerate(parts)
    ]


def exchange(x):
    return lax.all_to_all(x, "freq", split_axis=0, concat_axis=0, tiled=True)


def on_device(ring, response_real, response_imaginary, focus, initial, onset):
    blocks, groups = lax.axis_size("rec"), lax.axis_size("freq")
    freqs, rows, cols = response_real.shape
    half = focus.shape[2] // 2
    chunks = CHUNKS if (half // blocks) % CHUNKS == 0 else 1
    width = half // chunks
    each = width // blocks
    per = blocks // groups
    part = cols // groups
    place = [ring.index(k) for k in range(blocks)]
    inverse, forward = (jnp.asarray(m) for m in window_tables(freqs * groups))
    d = lax.axis_index("freq")

    turned = onset.T.reshape(chunks, blocks, each, rows)
    sent = jnp.stack([turned[:, place[k]] for k in range(blocks)])
    got = lax.all_to_all(sent, "rec", split_axis=0, concat_axis=0, tiled=True)
    source_onset = jnp.transpose(got, (1, 2, 0, 3)).reshape(chunks, each, cols)
    source_onset = lax.dynamic_slice_in_dim(source_onset, d * part, part, 2)
    own = lax.dynamic_slice_in_dim(turned.reshape(chunks, groups, per, each, rows), d, 1, 1)[:, 0]
    receiver_onset = jnp.transpose(own, (0, 2, 1, 3)).reshape(chunks, each, per * rows)

    partials = []
    for j in range(chunks):
        sums = adjoint_terms(response_real, response_imaginary, focus, j * width, width, blocks, groups)
        partials.append(
            lax.psum_scatter(sums, "rec", scatter_dimension=0, tiled=True, axis_index_groups=[ring])[0]
        )
    gathered = []
    for j in range(chunks):
        spectra = exchange(partials[j])
        returned = exchange(window(spectra, source_onset[j], inverse, forward))
        gathered.append(lax.all_gather(returned, "rec", axis=0, tiled=False, axis_index_groups=[ring]))
    relative = (per * each) % 8 == 0 and groups & (groups - 1) == 0
    index = d.astype(jnp.int32).reshape(1)
    pieces, strips = pieces_of(freqs), strips_of(freqs)
    updates = []
    after = []
    for j in range(chunks):
        spectra = [
            swap(relative, forward_terms(relative, index, response_real, response_imaginary, gathered[j], after, *piece))
            for piece in pieces
        ]
        clipped = window_pieces(relative, index, spectra, j, receiver_onset, inverse, forward, pieces, strips)
        updates.append([swap(relative, x) for x in clipped])
        after = [x for piece in updates[j] for x in piece]
    result = initial
    for h, strip in enumerate(strips):
        result = finish(relative, index, initial, result, [updates[j][h] for j in range(chunks)], *strip)
    return result


def solution(mesh):
    return jax.shard_map(
        functools.partial(on_device, ring_order(mesh)),
        mesh=mesh,
        in_specs=(
            P("freq", "rec", None),
            P("freq", "rec", None),
            P("rec", "freq", None),
            P("rec", "freq", None),
            P("rec", None),
        ),
        out_specs=P("rec", "freq", None),
        check_vma=False,
    )
```

```python
import functools
import math

import jax
import jax.numpy as jnp
import numpy as np
from jax import lax
from jax.experimental import pallas as pl
from jax.experimental.pallas import tpu as pltpu
from jax.sharding import PartitionSpec as P

CHUNKS = 2
DEPTH = 4
UNIT = 2
LARGE, SMALL = 52 << 20, 16 << 20
F32, BF16 = jnp.float32, jnp.bfloat16


def ring_order(mesh):
    axis = mesh.axis_names.index("rec")
    devices = np.moveaxis(mesh.devices, axis, 0).reshape(mesh.devices.shape[axis], -1)[:, 0]
    count = len(devices)
    try:
        spots = {tuple(d.coords[1:]): i for i, d in enumerate(devices)}
    except AttributeError:
        return list(range(count))
    ys = sorted({y for y, _ in spots})
    zs = sorted({z for _, z in spots})
    if len(spots) != count or len(ys) * len(zs) != count or len(ys) % 2 or len(zs) < 2:
        return list(range(count))
    path = [(y, zs[0]) for y in ys]
    for turn, y in enumerate(reversed(ys)):
        path += [(y, z) for z in (zs[1:] if turn % 2 == 0 else zs[:0:-1])]
    return [spots[p] for p in path]


def tiling(width):
    return (width // 128, 128) if width % 128 == 0 else (1, width)


def split(x):
    high = x.astype(BF16)
    return high, (x - high.astype(F32)).astype(BF16)


def dot(a, b, dims=((1,), (0,))):
    return lax.dot_general(a, b, (dims, ((), ())), preferred_element_type=F32)


def adjoint_kernel(start, width, groups, real_hbm, imag_hbm, x_ref, out_ref, real_ref, imag_ref, sems):
    f = pl.program_id(0)
    blocks, _, tiles, _, pair, lanes = out_ref.shape
    cols = tiles * lanes
    each = pair // 2
    half = x_ref.shape[2] // 2
    x = x_ref[:, pl.ds(f, 1), :].reshape(x_ref.shape[0], 2 * half).T
    re, im = x[start:start + width], x[half + start:half + start + width]
    left = jnp.concatenate([jnp.concatenate([re, im], 1), jnp.concatenate([im, -re], 1)], 0)
    high, low = split(left)
    left = jnp.concatenate(
        [jnp.concatenate([high, high], 1), jnp.concatenate([low, jnp.zeros_like(low)], 1)], 0
    )
    sources = [lambda n, ref=ref: ref.at[n] for ref in (real_hbm, imag_hbm)]
    slot, = stream(0, real_hbm.shape[0], 1, sources, (real_ref, imag_ref), sems)
    for g in range(groups):
        at = pl.ds(g * cols, cols)
        right = jnp.concatenate([real_ref[slot, :, at], imag_ref[slot, :, at]], 0)
        right = jnp.concatenate(split(right), 0)
        both = dot(left, right)
        total = both[: 2 * width] + both[2 * width:]
        for i in range(blocks):
            for c in range(2):
                row = c * width + i * each
                for t in range(tiles):
                    out_ref[i, g, t, 0, c * each:(c + 1) * each, :] = total[
                        row:row + each, t * lanes:(t + 1) * lanes
                    ]


def stream(first, count, unit, sources, buffers, sems):
    depth = buffers[0].shape[0]
    step = pl.program_id(0)
    ahead = min(depth - unit, count)

    def copies(f):
        slot = lax.rem(f, depth)
        return [
            pltpu.make_async_copy(source(f + first), buffer.at[slot], sems.at[n, slot])
            for n, (source, buffer) in enumerate(zip(sources, buffers))
        ]

    @pl.when(step == 0)
    def _():
        for f in range(ahead):
            for copy in copies(jnp.int32(f)):
                copy.start()

    for u in range(unit):
        later = step * unit + ahead + u

        @pl.when(later < count)
        def _():
            for copy in copies(later):
                copy.start()

    for u in range(unit):
        for copy in copies(step * unit + u):
            copy.wait()
    return [lax.rem(step * unit + u, depth) for u in range(unit)]


def unit_of(count):
    return UNIT if count % UNIT == 0 else 1


def adjoint_terms(real_part, imag_part, x, start, width, blocks, groups):
    freqs, rows, cols = real_part.shape
    each = width // blocks
    tiles, lanes = tiling(cols // groups)
    whole = pl.BlockSpec(memory_space=pl.ANY)
    return pl.pallas_call(
        functools.partial(adjoint_kernel, start, width, groups),
        grid=(freqs,),
        in_specs=[whole, whole, pl.BlockSpec(x.shape, lambda f: (0, 0, 0))],
        out_specs=pl.BlockSpec((blocks, groups, tiles, 1, 2 * each, lanes), lambda f: (0, 0, 0, f, 0, 0)),
        out_shape=jax.ShapeDtypeStruct((blocks, groups, tiles, freqs, 2 * each, lanes), F32),
        scratch_shapes=[pltpu.VMEM((DEPTH, rows, cols), F32)] * 2 + [pltpu.SemaphoreType.DMA((2, DEPTH))],
        compiler_params=pltpu.CompilerParams(dimension_semantics=("arbitrary",)),
        cost_estimate=pl.CostEstimate(
            flops=24 * width * freqs * rows * cols, bytes_accessed=8 * freqs * rows * cols, transcendentals=0
        ),
        name="adjoint",
    )(real_part, imag_part, x)


def window_kernel(x_ref, onset_ref, inv_ref, fwd_ref, out_ref):
    groups, tiles, _, lanes = x_ref.shape
    each = onset_ref.shape[0]
    order = x_ref.shape[2] // each
    inverse = inv_ref[...]
    forward = fwd_ref[...]
    samples = inv_ref.shape[0] // 2
    when = lax.broadcasted_iota(jnp.int32, (samples, tiles * lanes), 0)

    def rows(p):
        return pl.ds(p, order, stride=each) if each > 1 else pl.ds(0, order)

    def apply(matrix, value):
        count = matrix.shape[0] // 2
        high, low = split(value)
        both = dot(matrix, high)
        return both[:count] + both[count:] + dot(matrix[:count], low)

    for p in range(each):
        spectra = jnp.concatenate(
            [jnp.concatenate([x_ref[g, t, rows(p), :] for t in range(tiles)], 1) for g in range(groups)], 0
        )
        traces = apply(inverse, spectra)
        clipped = jnp.where(when < onset_ref[p:p + 1, :], traces, 0.0)
        back = apply(forward, clipped)
        for g in range(groups):
            for t in range(tiles):
                out_ref[g, t, rows(p), :] = back[g * order:(g + 1) * order, t * lanes:(t + 1) * lanes]


def window_tables(freqs):
    samples = 2 * freqs
    k, t = np.arange(freqs), np.arange(samples)
    phase = 2.0 * np.pi / samples * (k[:, None] * t[None, :] % samples)
    factor = np.where(k == 0, 1.0, 2.0)[:, None] / samples
    inverse = np.stack([factor * np.cos(phase), -factor * np.sin(phase)], 1)
    forward = np.stack([np.cos(phase), -np.sin(phase)], 1)
    inverse = inverse.reshape(2 * freqs, samples).T
    forward = forward.reshape(2 * freqs, samples)

    def stacked(m):
        m = m.astype(np.float32)
        high = m.astype(BF16)
        low = (m - high.astype(np.float32)).astype(BF16)
        return np.concatenate([high, low], 0)

    return stacked(inverse), stacked(forward)


def window(x, onset, inverse, forward):
    groups, tiles, freqs, pair, lanes = x.shape
    flat = x.reshape(groups, tiles, freqs * pair, lanes)
    vmem = pl.BlockSpec(memory_space=pltpu.VMEM)
    out = pl.pallas_call(
        window_kernel,
        out_shape=jax.ShapeDtypeStruct(flat.shape, F32),
        in_specs=[vmem] * 4,
        out_specs=vmem,
        cost_estimate=pl.CostEstimate(
            flops=24 * groups * freqs * flat.size, bytes_accessed=8 * flat.size, transcendentals=0
        ),
        compiler_params=pltpu.CompilerParams(vmem_limit_bytes=SMALL),
        name="window",
    )(flat, onset, inverse, forward)
    return out.reshape(x.shape)


def pieces_of(freqs):
    return [(0, freqs - 4), (freqs - 4, 4)] if freqs % 8 == 0 and freqs > 8 else [(0, freqs)]


def combine(total, rows, blocks, each):
    count = blocks * 2 * each
    high, low = total[:, :count], total[:, count:]
    parts = [high[n:n + rows] + low[n:n + rows] + high[n + rows:n + 2 * rows] for n in (0, 2 * rows)]
    both = jnp.concatenate(parts, 1).T
    first, second = both[:count], both[count:].reshape(blocks, 2 * each, rows)
    turned = jnp.concatenate([-second[:, each:], second[:, :each]], 1)
    return first + turned.reshape(count, rows)


def strips_of(freqs):
    return [(n, 8) for n in range(0, freqs, 8)] if freqs % 8 == 0 else [(0, freqs)]


def forward_kernel(relative, groups, first, shift, number, d_ref, real_hbm, imag_hbm, w_hbm, *refs):
    outs, (result_ref, real_ref, imag_ref, w_ref, sems) = refs[-5 - groups:-5], refs[-5:]
    unit = unit_of(number)
    sources = [lambda n, ref=ref: ref.at[n] for ref in (real_hbm, imag_hbm)]
    sources.append(lambda n: w_hbm.at[:, :, :, n - shift])
    slots = stream(first, number, unit, sources, (real_ref, imag_ref, w_ref), sems)
    _, blocks, _, tiles, pair, lanes = w_ref.shape
    part = tiles * lanes
    rows = real_hbm.shape[1]
    count = blocks * pair
    for u, slot in enumerate(slots):
        w = jnp.concatenate([w_ref[slot, :, g, t] for g in range(groups) for t in range(tiles)], 2)
        right = jnp.concatenate(split(w.reshape(count, groups * part)), 0)
        left = jnp.concatenate([*split(real_ref[slot]), *split(imag_ref[slot])], 0)
        result_ref[u] = combine(dot(left, right, ((1,), (1,))), rows, blocks, pair // 2)
    per = blocks // groups
    d = d_ref[0] if relative else 0
    for u in range(unit):
        for k, out_ref in enumerate(outs):
            out_tiles, _, _, out_lanes = out_ref.shape
            start = member(d, k, per * pair)
            value = result_ref[u, pl.ds(start, per * pair), :]
            wide = jnp.concatenate([value[i * pair:(i + 1) * pair] for i in range(per)], 1)
            for t in range(out_tiles):
                out_ref[t, pl.program_id(0) * unit + u] = wide[:, t * out_lanes:(t + 1) * out_lanes]


def member(d, k, size, offset=0):
    start = (d ^ k) * size + offset
    return start if isinstance(d, int) else pl.multiple_of(start, 8)


def forward_terms(relative, d, real_part, imag_part, w, shift, after, first, count):
    _, rows, cols = real_part.shape
    blocks, groups, tiles, _, pair, lanes = w.shape
    out_tiles, out_lanes = tiling(blocks // groups * rows)
    unit = unit_of(count)
    depth = DEPTH + unit - 1
    whole = pl.BlockSpec(memory_space=pl.ANY)
    return pl.pallas_call(
        functools.partial(forward_kernel, relative, groups, first, shift, count),
        grid=(count // unit,),
        in_specs=[pl.BlockSpec(memory_space=pltpu.SMEM)] + [whole] * (3 + len(after)),
        out_specs=[pl.BlockSpec((out_tiles, count, pair, out_lanes), lambda f: (0, 0, 0, 0))] * groups,
        out_shape=[jax.ShapeDtypeStruct((out_tiles, count, pair, out_lanes), F32)] * groups,
        scratch_shapes=[
            pltpu.VMEM((unit, blocks * pair, rows), F32),
            pltpu.VMEM((depth, rows, cols), F32),
            pltpu.VMEM((depth, rows, cols), F32),
            pltpu.VMEM((depth, blocks, groups, tiles, pair, lanes), F32),
            pltpu.SemaphoreType.DMA((3, depth)),
        ],
        compiler_params=pltpu.CompilerParams(dimension_semantics=("arbitrary",), vmem_limit_bytes=LARGE),
        cost_estimate=pl.CostEstimate(
            flops=12 * blocks * pair * count * rows * cols, bytes_accessed=8 * count * rows * cols, transcendentals=0
        ),
        name="forward",
    )(d, real_part, imag_part, w, *after)


def window_pieces_kernel(relative, groups, chunk, pieces, strips, d_ref, onset_ref, inv_ref, fwd_ref, *refs):
    number = groups * len(pieces)
    ins, outs, spectra_ref = refs[:number], refs[number:-1], refs[-1]
    tiles, _, lanes = ins[0].shape
    each = onset_ref.shape[1]
    freqs = sum(count for _, count in pieces)
    inverse = inv_ref[...]
    forward = fwd_ref[...]
    samples = inv_ref.shape[0] // 2
    when = lax.broadcasted_iota(jnp.int32, (samples, tiles * lanes), 0)
    d = d_ref[0] if relative else 0

    def apply(matrix, value):
        count = matrix.shape[0] // 2
        high, low = split(value)
        both = dot(matrix, high)
        return both[:count] + both[count:] + dot(matrix[:count], low)

    def places(cuts):
        return [
            (h * groups + k, pl.ds(member(d, k, 2 * freqs, 2 * first), 2 * count), 2 * count)
            for h, (first, count) in enumerate(cuts)
            for k in range(groups)
        ]

    for p in range(each):
        for n, place, order in places(pieces):
            rows = pl.ds(p, order, stride=each) if each > 1 else pl.ds(0, order)
            for t in range(tiles):
                spectra_ref[p, place, t * lanes:(t + 1) * lanes] = ins[n][t, rows, :]
        traces = apply(inverse, spectra_ref[p])
        clipped = jnp.where(when < onset_ref[chunk, p:p + 1, :], traces, 0.0)
        spectra_ref[p] = apply(forward, clipped)
        for n, place, order in places(strips):
            rows = pl.ds(p, order, stride=each) if each > 1 else pl.ds(0, order)
            for t in range(tiles):
                outs[n][t, rows, :] = spectra_ref[p, place, t * lanes:(t + 1) * lanes]


def window_pieces(relative, d, parts, chunk, onset, inverse, forward, pieces, strips):
    groups = len(parts[0])
    flat = [x.reshape(x.shape[0], -1, x.shape[3]) for piece in parts for x in piece]
    tiles, _, lanes = flat[0].shape
    each = onset.shape[1]
    vmem = pl.BlockSpec(memory_space=pltpu.VMEM)
    size = sum(x.size for x in flat)
    shapes = [(tiles, count, 2 * each, lanes) for _, count in strips for _ in range(groups)]
    flat_shapes = [jax.ShapeDtypeStruct((tiles, count * 2 * each, lanes), F32) for _, count, _, _ in shapes]
    out = pl.pallas_call(
        functools.partial(window_pieces_kernel, relative, groups, chunk, pieces, strips),
        out_shape=flat_shapes,
        in_specs=[pl.BlockSpec(memory_space=pltpu.SMEM)] + [vmem] * (3 + len(flat)),
        out_specs=[vmem] * len(shapes),
        scratch_shapes=[pltpu.VMEM((each, inverse.shape[1], tiles * lanes), F32)],
        cost_estimate=pl.CostEstimate(
            flops=12 * inverse.shape[1] * size, bytes_accessed=8 * size, transcendentals=0
        ),
        compiler_params=pltpu.CompilerParams(vmem_limit_bytes=SMALL),
        name="window",
    )(d, onset, inverse, forward, *flat)
    out = [x.reshape(shape) for x, shape in zip(out, shapes)]
    return [out[h * groups:(h + 1) * groups] for h in range(len(strips))]


def finish_kernel(relative, chunks, groups, d_ref, initial_ref, before_ref, *refs):
    del before_ref
    parts, out_ref, turned_ref = refs[:chunks * groups], refs[-2], refs[-1]
    tiles, freqs, pair, lanes = parts[0].shape
    rows, _, full = out_ref.shape
    each, per, half = pair // 2, tiles * lanes // rows, full // 2
    d = d_ref[0] if relative else 0
    for f in range(freqs):
        for j in range(chunks):
            for k in range(groups):
                part = parts[j * groups + k]
                value = jnp.concatenate([part[t, f] for t in range(tiles)], 1)
                for c in range(2):
                    block = jnp.concatenate(
                        [value[c * each:(c + 1) * each, i * rows:(i + 1) * rows] for i in range(per)], 0
                    )
                    start = member(d, k, per * each, c * half + j * half // chunks)
                    turned_ref[f, pl.ds(start, per * each), :] = block
        out_ref[:, f, :] = initial_ref[:, f, :] - turned_ref[f].T


def finish(relative, d, initial, before, parts, first, count):
    rows, freqs, full = initial.shape
    chunks, groups = len(parts), len(parts[0])
    vmem = pl.BlockSpec(memory_space=pltpu.VMEM)
    strip = pl.BlockSpec((rows, count, full), lambda i: (0, first // count, 0))
    return pl.pallas_call(
        functools.partial(finish_kernel, relative, chunks, groups),
        grid=(1,),
        out_shape=jax.ShapeDtypeStruct(initial.shape, F32),
        in_specs=[pl.BlockSpec(memory_space=pltpu.SMEM), strip, pl.BlockSpec(memory_space=pl.ANY)]
        + [vmem] * (chunks * groups),
        out_specs=strip,
        scratch_shapes=[pltpu.VMEM((count, full, rows), F32)],
        input_output_aliases={} if before is initial else {2: 0},
        compiler_params=pltpu.CompilerParams(vmem_limit_bytes=SMALL),
        name="finish",
    )(d, initial, before, *[x for part in parts for x in part])


def swap(relative, parts):
    groups = len(parts)
    if not relative:
        return list(exchange(jnp.stack(parts)))
    return [
        lax.ppermute(x, "freq", [(i, i ^ k) for i in range(groups)]) if k else x for k, x in enumerate(parts)
    ]


def exchange(x):
    return lax.all_to_all(x, "freq", split_axis=0, concat_axis=0, tiled=True)


def on_device(ring, response_real, response_imaginary, focus, initial, onset):
    blocks, groups = lax.axis_size("rec"), lax.axis_size("freq")
    freqs, rows, cols = response_real.shape
    half = focus.shape[2] // 2
    chunks = CHUNKS if (half // blocks) % CHUNKS == 0 else 1
    width = half // chunks
    each = width // blocks
    per = blocks // groups
    part = cols // groups
    place = [ring.index(k) for k in range(blocks)]
    inverse, forward = (jnp.asarray(m) for m in window_tables(freqs * groups))
    d = lax.axis_index("freq")

    turned = onset.T.reshape(chunks, blocks, each, rows)
    sent = jnp.stack([turned[:, place[k]] for k in range(blocks)])
    got = lax.all_to_all(sent, "rec", split_axis=0, concat_axis=0, tiled=True)
    source_onset = jnp.transpose(got, (1, 2, 0, 3)).reshape(chunks, each, cols)
    source_onset = lax.dynamic_slice_in_dim(source_onset, d * part, part, 2)
    own = lax.dynamic_slice_in_dim(turned.reshape(chunks, groups, per, each, rows), d, 1, 1)[:, 0]
    receiver_onset = jnp.transpose(own, (0, 2, 1, 3)).reshape(chunks, each, per * rows)

    partials = []
    for j in range(chunks):
        sums = adjoint_terms(response_real, response_imaginary, focus, j * width, width, blocks, groups)
        partials.append(
            lax.psum_scatter(sums, "rec", scatter_dimension=0, tiled=True, axis_index_groups=[ring])[0]
        )
    pieces, strips = pieces_of(freqs), strips_of(freqs)

    def gather(x):
        return lax.all_gather(x, "rec", axis=0, tiled=False, axis_index_groups=[ring])

    gathered = []
    for j in range(chunks):
        spectra = exchange(partials[j])
        returned = exchange(window(spectra, source_onset[j], inverse, forward))
        if j < chunks - 1:
            gathered.append([(gather(returned), 0)] * len(pieces))
        else:
            gathered.append([(gather(returned[:, :, n:n + m]), n) for n, m in pieces])
    relative = (per * each) % 8 == 0 and groups & (groups - 1) == 0
    index = d.astype(jnp.int32).reshape(1)
    updates = []
    after = []
    for j in range(chunks):
        spectra = [
            swap(relative, forward_terms(relative, index, response_real, response_imaginary, *got, after, *piece))
            for got, piece in zip(gathered[j], pieces)
        ]
        clipped = window_pieces(relative, index, spectra, j, receiver_onset, inverse, forward, pieces, strips)
        updates.append([swap(relative, x) for x in clipped])
        after = [x for piece in updates[j] for x in piece]
    result = initial
    for h, strip in enumerate(strips):
        result = finish(relative, index, initial, result, [updates[j][h] for j in range(chunks)], *strip)
    return result


def solution(mesh):
    return jax.shard_map(
        functools.partial(on_device, ring_order(mesh)),
        mesh=mesh,
        in_specs=(
            P("freq", "rec", None),
            P("freq", "rec", None),
            P("rec", "freq", None),
            P("rec", "freq", None),
            P("rec", None),
        ),
        out_specs=P("rec", "freq", None),
        check_vma=False,
    )
```

```python
import functools
import math

import jax
import jax.numpy as jnp
import numpy as np
from jax import lax
from jax.experimental import pallas as pl
from jax.experimental.pallas import tpu as pltpu
from jax.sharding import PartitionSpec as P

CHUNKS = 2
DEPTH = 4
UNIT = 2
LARGE, SMALL = 52 << 20, 16 << 20
F32, BF16 = jnp.float32, jnp.bfloat16


def ring_order(mesh):
    axis = mesh.axis_names.index("rec")
    devices = np.moveaxis(mesh.devices, axis, 0).reshape(mesh.devices.shape[axis], -1)[:, 0]
    count = len(devices)
    try:
        spots = {tuple(d.coords[1:]): i for i, d in enumerate(devices)}
    except AttributeError:
        return list(range(count))
    ys = sorted({y for y, _ in spots})
    zs = sorted({z for _, z in spots})
    if len(spots) != count or len(ys) * len(zs) != count or len(ys) % 2 or len(zs) < 2:
        return list(range(count))
    path = [(y, zs[0]) for y in ys]
    for turn, y in enumerate(reversed(ys)):
        path += [(y, z) for z in (zs[1:] if turn % 2 == 0 else zs[:0:-1])]
    return [spots[p] for p in path]


def tiling(width):
    return (width // 128, 128) if width % 128 == 0 else (1, width)


def split(x):
    high = x.astype(BF16)
    return high, (x - high.astype(F32)).astype(BF16)


def dot(a, b, dims=((1,), (0,))):
    return lax.dot_general(a, b, (dims, ((), ())), preferred_element_type=F32)


def adjoint_kernel(start, width, groups, real_hbm, imag_hbm, x_ref, out_ref, real_ref, imag_ref, sems):
    f = pl.program_id(0)
    blocks, _, tiles, _, pair, lanes = out_ref.shape
    cols = tiles * lanes
    each = pair // 2
    half = x_ref.shape[2] // 2
    x = x_ref[:, pl.ds(f, 1), :].reshape(x_ref.shape[0], 2 * half).T
    re, im = x[start:start + width], x[half + start:half + start + width]
    left = jnp.concatenate([jnp.concatenate([re, im], 1), jnp.concatenate([im, -re], 1)], 0)
    high, low = split(left)
    left = jnp.concatenate(
        [jnp.concatenate([high, high], 1), jnp.concatenate([low, jnp.zeros_like(low)], 1)], 0
    )
    sources = [lambda n, ref=ref: ref.at[n] for ref in (real_hbm, imag_hbm)]
    slot, = stream(0, real_hbm.shape[0], 1, sources, (real_ref, imag_ref), sems)
    for g in range(groups):
        at = pl.ds(g * cols, cols)
        right = jnp.concatenate([real_ref[slot, :, at], imag_ref[slot, :, at]], 0)
        right = jnp.concatenate(split(right), 0)
        both = dot(left, right)
        total = both[: 2 * width] + both[2 * width:]
        for i in range(blocks):
            for c in range(2):
                row = c * width + i * each
                for t in range(tiles):
                    out_ref[i, g, t, 0, c * each:(c + 1) * each, :] = total[
                        row:row + each, t * lanes:(t + 1) * lanes
                    ]


def stream(first, count, unit, sources, buffers, sems):
    depth = buffers[0].shape[0]
    step = pl.program_id(0)
    ahead = min(depth - unit, count)

    def copies(f):
        slot = lax.rem(f, depth)
        return [
            pltpu.make_async_copy(source(f + first), buffer.at[slot], sems.at[n, slot])
            for n, (source, buffer) in enumerate(zip(sources, buffers))
        ]

    @pl.when(step == 0)
    def _():
        for f in range(ahead):
            for copy in copies(jnp.int32(f)):
                copy.start()

    for u in range(unit):
        later = step * unit + ahead + u

        @pl.when(later < count)
        def _():
            for copy in copies(later):
                copy.start()

    for u in range(unit):
        for copy in copies(step * unit + u):
            copy.wait()
    return [lax.rem(step * unit + u, depth) for u in range(unit)]


def unit_of(count):
    return UNIT if count % UNIT == 0 else 1


def adjoint_terms(real_part, imag_part, x, start, width, blocks, groups):
    freqs, rows, cols = real_part.shape
    each = width // blocks
    tiles, lanes = tiling(cols // groups)
    whole = pl.BlockSpec(memory_space=pl.ANY)
    return pl.pallas_call(
        functools.partial(adjoint_kernel, start, width, groups),
        grid=(freqs,),
        in_specs=[whole, whole, pl.BlockSpec(x.shape, lambda f: (0, 0, 0))],
        out_specs=pl.BlockSpec((blocks, groups, tiles, 1, 2 * each, lanes), lambda f: (0, 0, 0, f, 0, 0)),
        out_shape=jax.ShapeDtypeStruct((blocks, groups, tiles, freqs, 2 * each, lanes), F32),
        scratch_shapes=[pltpu.VMEM((DEPTH, rows, cols), F32)] * 2 + [pltpu.SemaphoreType.DMA((2, DEPTH))],
        compiler_params=pltpu.CompilerParams(dimension_semantics=("arbitrary",)),
        cost_estimate=pl.CostEstimate(
            flops=24 * width * freqs * rows * cols, bytes_accessed=8 * freqs * rows * cols, transcendentals=0
        ),
        name="adjoint",
    )(real_part, imag_part, x)


def window_kernel(x_ref, onset_ref, inv_ref, fwd_ref, out_ref):
    groups, tiles, _, lanes = x_ref.shape
    each = onset_ref.shape[0]
    order = x_ref.shape[2] // each
    inverse = inv_ref[...]
    forward = fwd_ref[...]
    samples = inv_ref.shape[0] // 2
    when = lax.broadcasted_iota(jnp.int32, (samples, tiles * lanes), 0)

    def rows(p):
        return pl.ds(p, order, stride=each) if each > 1 else pl.ds(0, order)

    def apply(matrix, value):
        count = matrix.shape[0] // 2
        high, low = split(value)
        both = dot(matrix, high)
        return both[:count] + both[count:] + dot(matrix[:count], low)

    for p in range(each):
        spectra = jnp.concatenate(
            [jnp.concatenate([x_ref[g, t, rows(p), :] for t in range(tiles)], 1) for g in range(groups)], 0
        )
        traces = apply(inverse, spectra)
        clipped = jnp.where(when < onset_ref[p:p + 1, :], traces, 0.0)
        back = apply(forward, clipped)
        for g in range(groups):
            for t in range(tiles):
                out_ref[g, t, rows(p), :] = back[g * order:(g + 1) * order, t * lanes:(t + 1) * lanes]


def window_tables(freqs):
    samples = 2 * freqs
    k, t = np.arange(freqs), np.arange(samples)
    phase = 2.0 * np.pi / samples * (k[:, None] * t[None, :] % samples)
    factor = np.where(k == 0, 1.0, 2.0)[:, None] / samples
    inverse = np.stack([factor * np.cos(phase), -factor * np.sin(phase)], 1)
    forward = np.stack([np.cos(phase), -np.sin(phase)], 1)
    inverse = inverse.reshape(2 * freqs, samples).T
    forward = forward.reshape(2 * freqs, samples)

    def stacked(m):
        m = m.astype(np.float32)
        high = m.astype(BF16)
        low = (m - high.astype(np.float32)).astype(BF16)
        return np.concatenate([high, low], 0)

    return stacked(inverse), stacked(forward)


def window(x, onset, inverse, forward):
    groups, tiles, freqs, pair, lanes = x.shape
    flat = x.reshape(groups, tiles, freqs * pair, lanes)
    vmem = pl.BlockSpec(memory_space=pltpu.VMEM)
    out = pl.pallas_call(
        window_kernel,
        out_shape=jax.ShapeDtypeStruct(flat.shape, F32),
        in_specs=[vmem] * 4,
        out_specs=vmem,
        cost_estimate=pl.CostEstimate(
            flops=24 * groups * freqs * flat.size, bytes_accessed=8 * flat.size, transcendentals=0
        ),
        compiler_params=pltpu.CompilerParams(vmem_limit_bytes=SMALL),
        name="window",
    )(flat, onset, inverse, forward)
    return out.reshape(x.shape)


def pieces_of(freqs):
    return [(0, freqs - 8), (freqs - 8, 8)] if freqs % 8 == 0 and freqs > 8 else [(0, freqs)]


def combine(total, rows, blocks, each):
    count = blocks * 2 * each
    high, low = total[:, :count], total[:, count:]
    parts = [high[n:n + rows] + low[n:n + rows] + high[n + rows:n + 2 * rows] for n in (0, 2 * rows)]
    both = jnp.concatenate(parts, 1).T
    first, second = both[:count], both[count:].reshape(blocks, 2 * each, rows)
    turned = jnp.concatenate([-second[:, each:], second[:, :each]], 1)
    return first + turned.reshape(count, rows)


def strips_of(freqs):
    return [(n, 8) for n in range(0, freqs, 8)] if freqs % 8 == 0 else [(0, freqs)]


def forward_kernel(relative, groups, first, shift, number, d_ref, real_hbm, imag_hbm, w_hbm, *refs):
    outs, (result_ref, real_ref, imag_ref, w_ref, sems) = refs[-5 - groups:-5], refs[-5:]
    unit = unit_of(number)
    sources = [lambda n, ref=ref: ref.at[n] for ref in (real_hbm, imag_hbm)]
    sources.append(lambda n: w_hbm.at[:, :, :, n - shift])
    slots = stream(first, number, unit, sources, (real_ref, imag_ref, w_ref), sems)
    _, blocks, _, tiles, pair, lanes = w_ref.shape
    part = tiles * lanes
    rows = real_hbm.shape[1]
    count = blocks * pair
    for u, slot in enumerate(slots):
        w = jnp.concatenate([w_ref[slot, :, g, t] for g in range(groups) for t in range(tiles)], 2)
        right = jnp.concatenate(split(w.reshape(count, groups * part)), 0)
        left = jnp.concatenate([*split(real_ref[slot]), *split(imag_ref[slot])], 0)
        result_ref[u] = combine(dot(left, right, ((1,), (1,))), rows, blocks, pair // 2)
    per = blocks // groups
    d = d_ref[0] if relative else 0
    for u in range(unit):
        for k, out_ref in enumerate(outs):
            out_tiles, _, _, out_lanes = out_ref.shape
            start = member(d, k, per * pair)
            value = result_ref[u, pl.ds(start, per * pair), :]
            wide = jnp.concatenate([value[i * pair:(i + 1) * pair] for i in range(per)], 1)
            for t in range(out_tiles):
                out_ref[t, pl.program_id(0) * unit + u] = wide[:, t * out_lanes:(t + 1) * out_lanes]


def member(d, k, size, offset=0):
    start = (d ^ k) * size + offset
    return start if isinstance(d, int) else pl.multiple_of(start, 8)


def forward_terms(relative, d, real_part, imag_part, w, shift, after, first, count):
    _, rows, cols = real_part.shape
    blocks, groups, tiles, _, pair, lanes = w.shape
    out_tiles, out_lanes = tiling(blocks // groups * rows)
    unit = unit_of(count)
    depth = DEPTH + unit - 1
    whole = pl.BlockSpec(memory_space=pl.ANY)
    return pl.pallas_call(
        functools.partial(forward_kernel, relative, groups, first, shift, count),
        grid=(count // unit,),
        in_specs=[pl.BlockSpec(memory_space=pltpu.SMEM)] + [whole] * (3 + len(after)),
        out_specs=[pl.BlockSpec((out_tiles, count, pair, out_lanes), lambda f: (0, 0, 0, 0))] * groups,
        out_shape=[jax.ShapeDtypeStruct((out_tiles, count, pair, out_lanes), F32)] * groups,
        scratch_shapes=[
            pltpu.VMEM((unit, blocks * pair, rows), F32),
            pltpu.VMEM((depth, rows, cols), F32),
            pltpu.VMEM((depth, rows, cols), F32),
            pltpu.VMEM((depth, blocks, groups, tiles, pair, lanes), F32),
            pltpu.SemaphoreType.DMA((3, depth)),
        ],
        compiler_params=pltpu.CompilerParams(dimension_semantics=("arbitrary",), vmem_limit_bytes=LARGE),
        cost_estimate=pl.CostEstimate(
            flops=12 * blocks * pair * count * rows * cols, bytes_accessed=8 * count * rows * cols, transcendentals=0
        ),
        name="forward",
    )(d, real_part, imag_part, w, *after)


def window_pieces_kernel(relative, groups, chunk, pieces, strips, d_ref, onset_ref, inv_ref, fwd_ref, *refs):
    number = groups * len(pieces)
    ins, outs, spectra_ref = refs[:number], refs[number:-1], refs[-1]
    tiles, _, lanes = ins[0].shape
    each = onset_ref.shape[1]
    freqs = sum(count for _, count in pieces)
    inverse = inv_ref[...]
    forward = fwd_ref[...]
    samples = inv_ref.shape[0] // 2
    when = lax.broadcasted_iota(jnp.int32, (samples, tiles * lanes), 0)
    d = d_ref[0] if relative else 0

    def apply(matrix, value):
        count = matrix.shape[0] // 2
        high, low = split(value)
        both = dot(matrix, high)
        return both[:count] + both[count:] + dot(matrix[:count], low)

    def places(cuts):
        return [
            (h * groups + k, pl.ds(member(d, k, 2 * freqs, 2 * first), 2 * count), 2 * count)
            for h, (first, count) in enumerate(cuts)
            for k in range(groups)
        ]

    for p in range(each):
        for n, place, order in places(pieces):
            rows = pl.ds(p, order, stride=each) if each > 1 else pl.ds(0, order)
            for t in range(tiles):
                spectra_ref[p, place, t * lanes:(t + 1) * lanes] = ins[n][t, rows, :]
        traces = apply(inverse, spectra_ref[p])
        clipped = jnp.where(when < onset_ref[chunk, p:p + 1, :], traces, 0.0)
        spectra_ref[p] = apply(forward, clipped)
        for n, place, order in places(strips):
            rows = pl.ds(p, order, stride=each) if each > 1 else pl.ds(0, order)
            for t in range(tiles):
                outs[n][t, rows, :] = spectra_ref[p, place, t * lanes:(t + 1) * lanes]


def window_pieces(relative, d, parts, chunk, onset, inverse, forward, pieces, strips):
    groups = len(parts[0])
    flat = [x.reshape(x.shape[0], -1, x.shape[3]) for piece in parts for x in piece]
    tiles, _, lanes = flat[0].shape
    each = onset.shape[1]
    vmem = pl.BlockSpec(memory_space=pltpu.VMEM)
    size = sum(x.size for x in flat)
    shapes = [(tiles, count, 2 * each, lanes) for _, count in strips for _ in range(groups)]
    flat_shapes = [jax.ShapeDtypeStruct((tiles, count * 2 * each, lanes), F32) for _, count, _, _ in shapes]
    out = pl.pallas_call(
        functools.partial(window_pieces_kernel, relative, groups, chunk, pieces, strips),
        out_shape=flat_shapes,
        in_specs=[pl.BlockSpec(memory_space=pltpu.SMEM)] + [vmem] * (3 + len(flat)),
        out_specs=[vmem] * len(shapes),
        scratch_shapes=[pltpu.VMEM((each, inverse.shape[1], tiles * lanes), F32)],
        cost_estimate=pl.CostEstimate(
            flops=12 * inverse.shape[1] * size, bytes_accessed=8 * size, transcendentals=0
        ),
        compiler_params=pltpu.CompilerParams(vmem_limit_bytes=SMALL),
        name="window",
    )(d, onset, inverse, forward, *flat)
    out = [x.reshape(shape) for x, shape in zip(out, shapes)]
    return [out[h * groups:(h + 1) * groups] for h in range(len(strips))]


def finish_kernel(relative, chunks, groups, d_ref, initial_ref, before_ref, *refs):
    del before_ref
    parts, out_ref, turned_ref = refs[:chunks * groups], refs[-2], refs[-1]
    tiles, freqs, pair, lanes = parts[0].shape
    rows, _, full = out_ref.shape
    each, per, half = pair // 2, tiles * lanes // rows, full // 2
    d = d_ref[0] if relative else 0
    for f in range(freqs):
        for j in range(chunks):
            for k in range(groups):
                part = parts[j * groups + k]
                value = jnp.concatenate([part[t, f] for t in range(tiles)], 1)
                for c in range(2):
                    block = jnp.concatenate(
                        [value[c * each:(c + 1) * each, i * rows:(i + 1) * rows] for i in range(per)], 0
                    )
                    start = member(d, k, per * each, c * half + j * half // chunks)
                    turned_ref[f, pl.ds(start, per * each), :] = block
        out_ref[:, f, :] = initial_ref[:, f, :] - turned_ref[f].T


def finish(relative, d, initial, before, parts, first, count):
    rows, freqs, full = initial.shape
    chunks, groups = len(parts), len(parts[0])
    vmem = pl.BlockSpec(memory_space=pltpu.VMEM)
    strip = pl.BlockSpec((rows, count, full), lambda i: (0, first // count, 0))
    return pl.pallas_call(
        functools.partial(finish_kernel, relative, chunks, groups),
        grid=(1,),
        out_shape=jax.ShapeDtypeStruct(initial.shape, F32),
        in_specs=[pl.BlockSpec(memory_space=pltpu.SMEM), strip, pl.BlockSpec(memory_space=pl.ANY)]
        + [vmem] * (chunks * groups),
        out_specs=strip,
        scratch_shapes=[pltpu.VMEM((count, full, rows), F32)],
        input_output_aliases={} if before is initial else {2: 0},
        compiler_params=pltpu.CompilerParams(vmem_limit_bytes=SMALL),
        name="finish",
    )(d, initial, before, *[x for part in parts for x in part])


def swap(relative, parts):
    groups = len(parts)
    if not relative:
        return list(exchange(jnp.stack(parts)))
    return [
        lax.ppermute(x, "freq", [(i, i ^ k) for i in range(groups)]) if k else x for k, x in enumerate(parts)
    ]


def exchange(x):
    return lax.all_to_all(x, "freq", split_axis=0, concat_axis=0, tiled=True)


def on_device(ring, response_real, response_imaginary, focus, initial, onset):
    blocks, groups = lax.axis_size("rec"), lax.axis_size("freq")
    freqs, rows, cols = response_real.shape
    half = focus.shape[2] // 2
    chunks = CHUNKS if (half // blocks) % CHUNKS == 0 else 1
    width = half // chunks
    each = width // blocks
    per = blocks // groups
    part = cols // groups
    place = [ring.index(k) for k in range(blocks)]
    inverse, forward = (jnp.asarray(m) for m in window_tables(freqs * groups))
    d = lax.axis_index("freq")

    turned = onset.T.reshape(chunks, blocks, each, rows)
    sent = jnp.stack([turned[:, place[k]] for k in range(blocks)])
    got = lax.all_to_all(sent, "rec", split_axis=0, concat_axis=0, tiled=True)
    source_onset = jnp.transpose(got, (1, 2, 0, 3)).reshape(chunks, each, cols)
    source_onset = lax.dynamic_slice_in_dim(source_onset, d * part, part, 2)
    own = lax.dynamic_slice_in_dim(turned.reshape(chunks, groups, per, each, rows), d, 1, 1)[:, 0]
    receiver_onset = jnp.transpose(own, (0, 2, 1, 3)).reshape(chunks, each, per * rows)

    partials = []
    for j in range(chunks):
        sums = adjoint_terms(response_real, response_imaginary, focus, j * width, width, blocks, groups)
        partials.append(
            lax.psum_scatter(sums, "rec", scatter_dimension=0, tiled=True, axis_index_groups=[ring])[0]
        )
    pieces, strips = pieces_of(freqs), strips_of(freqs)

    def gather(x):
        return lax.all_gather(x, "rec", axis=0, tiled=False, axis_index_groups=[ring])

    gathered = []
    for j in range(chunks):
        spectra = exchange(partials[j])
        returned = exchange(window(spectra, source_onset[j], inverse, forward))
        if j < chunks - 1:
            gathered.append([(gather(returned), 0)] * len(pieces))
        else:
            gathered.append([(gather(returned[:, :, n:n + m]), n) for n, m in pieces])
    relative = (per * each) % 8 == 0 and groups & (groups - 1) == 0
    index = d.astype(jnp.int32).reshape(1)
    updates = []
    after = []
    for j in range(chunks):
        spectra = [
            swap(relative, forward_terms(relative, index, response_real, response_imaginary, *got, after, *piece))
            for got, piece in zip(gathered[j], pieces)
        ]
        clipped = window_pieces(relative, index, spectra, j, receiver_onset, inverse, forward, pieces, strips)
        updates.append([swap(relative, x) for x in clipped])
        after = [x for piece in updates[j] for x in piece]
    result = initial
    for h, strip in enumerate(strips):
        result = finish(relative, index, initial, result, [updates[j][h] for j in range(chunks)], *strip)
    return result


def solution(mesh):
    return jax.shard_map(
        functools.partial(on_device, ring_order(mesh)),
        mesh=mesh,
        in_specs=(
            P("freq", "rec", None),
            P("freq", "rec", None),
            P("rec", "freq", None),
            P("rec", "freq", None),
            P("rec", None),
        ),
        out_specs=P("rec", "freq", None),
        check_vma=False,
    )
```
